32 devices in a mesh: row: 4 (over y, x), col: 8 (over z, core).
Axes of the slice: x: 2, y: 2, z: 4, core: 2. Of those that a mesh axis runs over, the one named last changes fastest.
Arguments:
- object_field: float32 [2, 1024, 2048], P(None, 'row', 'col'), may hold values from -40 to 40
- probe: float32 [2, 4, 256, 256], replicated, may hold values from -3 to 3
- pos_rows: int32 [4, 8, 2, 3], P('row', 'col'), may hold values from 0 to 255
- pos_cols: int32 [4, 8, 2, 3], P('row', 'col'), may hold values from 0 to 255
- counts: int32 [4, 8, 2], P('row', 'col'), may hold values from 1 to 3, as said below
- magnitudes: float32 [4, 8, 2, 3, 256, 256], P('row', 'col'), may hold values from 0 to 4
Outputs:
- object_out: float32 [2, 1024, 2048], P(None, 'row', 'col')
- probe_out: float32 [2, 4, 256, 256], replicated
- errors: float32 [4], replicated
The draws below stay inside these ranges and needn't reach their ends.
Inputs may be any that keep to these rules, and one draw needn't show every extreme that they name: `counts`: every tile holds at least one live position in each batch, and in every batch some tile holds 3.
All inputs are finite; a program needn't handle non-finite values.
Results may differ from the reference program's by a relative error of at most 0.0015.
Values sent between devices are 32-bit elements; how exact they have to be, the bound alone decides.
A program may use at most 128 MiB of HBM per device.

```python
import math
import jax
import jax.numpy as jnp
from jax import lax

PROBE = 256
MODES = 4
TILE = 256
SLOTS = 3
BATCHES = 2
ITERS = 2
HALO = 128
GRID_ROWS = 4
GRID_COLS = 8
NX = 1024
NY = 2048


def draw_object_field(key, part):
    keys = jax.random.split(key, 1)
    base = jnp.clip(jax.random.normal(keys[0], (2, NX, NY), jnp.float32), -6.0, 6.0)
    col_scale = jnp.exp(jnp.linspace(math.log(0.6), math.log(1.8), NY)).astype(jnp.float32)
    return base * col_scale[None, None, :]


def draw_counts(key, part):
    keys = jax.random.split(key, 2)
    level = jax.random.randint(keys[0], (GRID_ROWS * GRID_COLS, BATCHES), 0, 10)
    middle = (SLOTS + 1) // 2
    filled = jnp.where(level >= 8, SLOTS, jnp.where(level >= 5, middle, 1)).astype(jnp.int32)
    chosen = jax.random.randint(keys[1], (BATCHES,), 0, GRID_ROWS * GRID_COLS)
    filled = filled.at[chosen, jnp.arange(BATCHES)].set(SLOTS)
    return filled.reshape(GRID_ROWS, GRID_COLS, BATCHES).astype(jnp.int32)


def with_ends(result, own_key, smallest, top_value):
    longest = result.shape.index(max(result.shape))
    spots = []
    for shift in (0, 1):
        where = [jax.random.randint(jax.random.fold_in(own_key, axis), (), 0, length) for axis, length in enumerate(result.shape)]
        where[longest] = (where[longest] + shift) % result.shape[longest]
        spots.append(tuple(where))
    return result.at[spots[0]].set(smallest).at[spots[1]].set(top_value)


def steps_of(rng, shape, pieces, smallest, top_value):
    def one(position, blocks):
        steps = jax.random.uniform(jax.random.fold_in(jax.random.fold_in(rng, 6), position), (blocks,), jnp.float32, smallest / len(pieces), top_value / len(pieces))
        return jnp.repeat(jnp.exp(steps), shape[position] // blocks).reshape((-1,) + (1,) * (len(shape) - position - 1))

    level = one(*pieces[0])
    for cut in pieces[1:]:
        level = level * one(*cut)
    return level


def bell_draw(own_key, dims, spread, bound, held_as=jnp.bfloat16):
    values = jax.random.normal(own_key, dims, jnp.float32) * spread
    return jnp.minimum(jnp.maximum(values, -bound), bound).astype(held_as)


def setup_inputs(seed: int = 0) -> dict:
    streams_of = jax.random.split(jax.random.key(seed), 7)
    object_field = draw_object_field(jax.random.fold_in(streams_of[6], 71), 0)
    probe = bell_draw(streams_of[1], (2, MODES, PROBE, PROBE), 0.5, 3.0, jnp.float32)
    pos_rows = with_ends(jax.random.randint(streams_of[2], (GRID_ROWS, GRID_COLS, BATCHES, SLOTS), 0, TILE), jax.random.fold_in(streams_of[2], 1), 0, TILE - 1).astype(jnp.int32)
    pos_cols = with_ends(jax.random.randint(streams_of[3], (GRID_ROWS, GRID_COLS, BATCHES, SLOTS), 0, TILE), jax.random.fold_in(streams_of[3], 1), 0, TILE - 1).astype(jnp.int32)
    counts = draw_counts(jax.random.fold_in(streams_of[6], 71), 0)
    magnitudes = jnp.clip(4.0 * jax.random.uniform(streams_of[5], (GRID_ROWS, GRID_COLS, BATCHES, SLOTS, PROBE, PROBE), jnp.float32) ** steps_of(streams_of[5], (GRID_ROWS, GRID_COLS, BATCHES, SLOTS, PROBE, PROBE), ((0, 4), (1, 8)), -0.2, 0.2), 0.0, 4.0)
    return {"object_field": object_field, "probe": probe, "pos_rows": pos_rows, "pos_cols": pos_cols, "counts": counts, "magnitudes": magnitudes}


object_rate = 0.9
probe_rate = 0.5
floor_value = 0.5
tiny_value = 1e-06

def dft_tables(probe_side):
    indices = jnp.arange(probe_side, dtype=jnp.int32)
    phase_index = indices[:, None] * indices[None, :] % probe_side
    angles = phase_index.astype(jnp.float32) * (2.0 * math.pi / probe_side)
    norm_scale = 1.0 / math.sqrt(probe_side)
    cosine = jnp.cos(angles) * norm_scale
    sine_part = -jnp.sin(angles) * norm_scale
    forward = jnp.stack([jnp.stack([cosine, -sine_part]), jnp.stack([sine_part, cosine])]).astype(jnp.bfloat16)
    inverse = jnp.stack([jnp.stack([cosine, sine_part]), jnp.stack([-sine_part, cosine])]).astype(jnp.bfloat16)
    return (forward, inverse)

def transform(field, table):
    table_wide = table.astype(jnp.float32)
    left_half = jnp.einsum('oixa,imab->omxb', table_wide, field.astype(jnp.float32)).astype(jnp.bfloat16)
    return jnp.einsum('imxb,oiby->omxy', left_half.astype(jnp.float32), table_wide)

def position_terms(window, probe, amplitude, forward, inverse):
    probe_re = probe[0]
    probe_im = probe[1]
    window_re = window[0][None]
    window_im = window[1][None]
    exit_wave = jnp.stack([probe_re * window_re - probe_im * window_im, probe_re * window_im + probe_im * window_re]).astype(jnp.bfloat16)
    far_field = transform(exit_wave, forward)
    modulus = jnp.sqrt(lax.optimization_barrier(jnp.sum(far_field * far_field, axis=(0, 1))))
    factor = amplitude / jnp.maximum(modulus, floor_value) - 1.0
    correction = (far_field * factor[None, None]).astype(jnp.bfloat16)
    update_wave = transform(correction, inverse)
    wave_re = update_wave[0]
    wave_im = update_wave[1]
    object_term = jnp.stack([lax.optimization_barrier(jnp.sum(probe_re * wave_re + probe_im * wave_im, axis=0)), lax.optimization_barrier(jnp.sum(probe_re * wave_im - probe_im * wave_re, axis=0))])
    probe_term = jnp.stack([window_re * wave_re + window_im * wave_im, window_re * wave_im - window_im * wave_re])
    power_term = jnp.sum(window * window)
    misfit = jnp.sum(jnp.square(modulus - amplitude))
    return (object_term, probe_term, power_term, misfit)

def reference(object_field, probe, pos_rows, pos_cols, counts, magnitudes):
    forward, inverse = dft_tables(PROBE)
    errors = []
    entries = jnp.arange(GRID_ROWS * GRID_COLS * SLOTS, dtype=jnp.int32)
    for sweep in range(ITERS):
        for batch in range(BATCHES):
            padded = jnp.pad(object_field, ((0, 0), (HALO, HALO), (HALO, HALO)))

            def step(carry, entry):
                object_grad, probe_grad, power_sum, misfit_sum = carry
                tile_row = entry // (GRID_COLS * SLOTS)
                tile_col = entry // SLOTS % GRID_COLS
                slot_index = entry % SLOTS
                live_mask = (slot_index < counts[tile_row, tile_col, batch]).astype(jnp.float32)
                corner_row = (tile_row * TILE + pos_rows[tile_row, tile_col, batch, slot_index]).astype(jnp.int32)
                corner_col = (tile_col * TILE + pos_cols[tile_row, tile_col, batch, slot_index]).astype(jnp.int32)
                anchor = (jnp.int32(0), corner_row, corner_col)
                window = lax.dynamic_slice(padded, anchor, (2, PROBE, PROBE))
                amplitude = magnitudes[tile_row, tile_col, batch, slot_index]
                object_term, probe_term, power_term, misfit = position_terms(window, probe, amplitude, forward, inverse)
                region = lax.dynamic_slice(object_grad, anchor, (2, PROBE, PROBE))
                object_grad = lax.dynamic_update_slice(object_grad, region + live_mask * object_term, anchor)
                return ((object_grad, probe_grad + live_mask * probe_term, power_sum + live_mask * power_term, misfit_sum + live_mask * misfit), None)
            start = (jnp.zeros(padded.shape, jnp.float32), jnp.zeros(probe.shape, jnp.float32), jnp.float32(0.0), jnp.float32(0.0))
            (object_grad, probe_grad, power_sum, misfit_sum), unused = lax.scan(step, start, entries)
            probe_peak = jnp.max(lax.optimization_barrier(jnp.sum(probe * probe, axis=(0, 1)))) + tiny_value
            object_field = object_field + object_rate / probe_peak * object_grad[:, HALO:HALO + NX, HALO:HALO + NY]
            probe = probe + probe_rate * PROBE * PROBE * probe_grad / power_sum
            errors.append(misfit_sum)
    return (object_field, probe, jnp.stack(errors))
```

```python
import functools
import math

import jax
import jax.numpy as jnp
import numpy as np
from jax import lax
from jax.experimental import pallas as pl
from jax.experimental.pallas import tpu as pltpu
from jax.sharding import PartitionSpec as P

BATCHES = 2
ITERS = 2


object_rate = 0.9
probe_rate = 0.5
floor_value = 0.5
tiny_value = 1e-06

CHUNK = 64
LANES = 128
SUBLANES = 8


def shifted(value, axis, steps):
    count = lax.axis_size(axis)
    leading, last = (max(0, -steps), min(count, count - steps))
    return lax.ppermute(value, axis, [(source, source + steps) for source in range(leading, last)])


def padded(array, sides, width):
    for axis, dim in sides:
        length = array.shape[dim]
        last = lax.slice_in_dim(array, length - width, length, axis=dim)
        leading = lax.slice_in_dim(array, 0, width, axis=dim)
        before = shifted(last, axis, 1)
        after = shifted(leading, axis, -1)
        array = jnp.concatenate([before, array, after], axis=dim)
    return array


def dft_tables(side):
    index = np.arange(side)
    angles = (index[:, None] * index[None, :] % side) * (2.0 * math.pi / side)
    cosine = np.cos(angles) / math.sqrt(side)
    sine = np.sin(angles) / math.sqrt(side)
    forward_left = np.block([[cosine, sine], [-sine, cosine]])
    inverse_left = np.block([[cosine, -sine], [sine, cosine]])
    return (jnp.asarray(forward_left, jnp.bfloat16), jnp.asarray(inverse_left, jnp.bfloat16))


def batch_kernel(
    rows_ref, cols_ref, count_ref, ext_ref, probe_ref, mag_ref, fwd_ref, inv_ref,
    grad_ref, sums_ref, win, far, term, square,
):
    modes, side = probe_ref.shape[1], probe_ref.shape[2]
    wide, tall = side + LANES, CHUNK + SUBLANES
    tail = 2 * modes * side

    grad_ref[...] = jnp.zeros_like(grad_ref)
    sums_ref[...] = jnp.zeros_like(sums_ref)

    def visit(slot, carry):
        row, col = rows_ref[slot], cols_ref[slot]
        first = pl.multiple_of(row // SUBLANES * SUBLANES, SUBLANES)
        down = row - first
        block = pl.multiple_of(col // LANES * LANES, LANES)
        offset = col - block

        for comp in range(2):
            for start in range(0, side, CHUNK):
                piece = ext_ref[comp, pl.ds(first + start, tall), pl.ds(block, wide)]
                piece = pltpu.roll(piece, lax.rem(wide - offset, wide), 1)[:, :side]
                piece = pltpu.roll(piece, lax.rem(tall - down, tall), 0)[:CHUNK]
                win[comp, start : start + CHUNK, :] = piece
                power = jnp.sum(piece * piece, axis=0, keepdims=True)
                sums_ref[tail : tail + 1, :] += power

        for mode in range(modes):
            p_re, p_im = probe_ref[0, mode], probe_ref[1, mode]
            w_re, w_im = win[0], win[1]
            wave = jnp.concatenate(
                [
                    (p_re * w_re - p_im * w_im).astype(jnp.bfloat16),
                    (p_re * w_im + p_im * w_re).astype(jnp.bfloat16),
                ],
                axis=0,
            )
            half = jnp.dot(fwd_ref[...], wave, preferred_element_type=jnp.float32).astype(jnp.bfloat16)
            half = jnp.concatenate([half[:side], half[side:]], axis=1)
            field = jnp.dot(half, inv_ref[...], preferred_element_type=jnp.float32)
            far[mode] = field
            norm = field[:, :side] * field[:, :side] + field[:, side:] * field[:, side:]
            if mode == 0:
                square[...] = norm
            else:
                square[...] += norm

        for start in range(0, side, CHUNK):
            span = slice(start, start + CHUNK)
            modulus = jnp.sqrt(square[span, :])
            amplitude = mag_ref[slot, span, :]
            miss = modulus - amplitude
            sums_ref[tail + 1 : tail + 2, :] += jnp.sum(miss * miss, axis=0, keepdims=True)
            square[span, :] = amplitude / jnp.maximum(modulus, floor_value) - 1.0

        for mode in range(modes):
            factor = square[...]
            fix = jnp.concatenate(
                [
                    (far[mode, :, :side] * factor).astype(jnp.bfloat16),
                    (far[mode, :, side:] * factor).astype(jnp.bfloat16),
                ],
                axis=0,
            )
            half = jnp.dot(inv_ref[...], fix, preferred_element_type=jnp.float32).astype(jnp.bfloat16)
            half = jnp.concatenate([half[:side], half[side:]], axis=1)
            wave = jnp.dot(half, fwd_ref[...], preferred_element_type=jnp.float32)
            u_re, u_im = wave[:, :side], wave[:, side:]
            p_re, p_im = probe_ref[0, mode], probe_ref[1, mode]
            w_re, w_im = win[0], win[1]
            t_re = p_re * u_re + p_im * u_im
            t_im = p_re * u_im - p_im * u_re
            if mode == 0:
                term[0, :, :side] = t_re
                term[1, :, :side] = t_im
            else:
                term[0, :, :side] += t_re
                term[1, :, :side] += t_im
            at_re, at_im = mode * side, (modes + mode) * side
            sums_ref[at_re : at_re + side, :] += w_re * u_re + w_im * u_im
            sums_ref[at_im : at_im + side, :] += w_re * u_im - w_im * u_re

        for comp in range(2):
            for start in range(0, side, CHUNK):
                piece = term[comp, start : start + CHUNK, :]
                piece = pltpu.roll(piece, offset, 1)
                piece = jnp.concatenate([piece, jnp.zeros((SUBLANES, wide), jnp.float32)], axis=0)
                piece = pltpu.roll(piece, down, 0)
                grad_ref[comp, pl.ds(first + start, tall), pl.ds(block, wide)] += piece
        return carry

    term[:, :, side:] = jnp.zeros((2, side, LANES), jnp.float32)
    lax.fori_loop(0, count_ref[0], visit, 0)


def batch_sums(extended, probe, rows, cols, count, magnitudes, forward, inverse):
    modes, side = probe.shape[1], probe.shape[2]
    vmem = pl.BlockSpec(memory_space=pltpu.VMEM)
    smem = pl.BlockSpec(memory_space=pltpu.SMEM)
    flops = 2 * magnitudes.shape[0] * modes * 4 * 2 * side * side * 4 * side
    return pl.pallas_call(
        batch_kernel,
        out_shape=(
            jax.ShapeDtypeStruct(extended.shape, jnp.float32),
            jax.ShapeDtypeStruct((2 * modes * side + 8, side), jnp.float32),
        ),
        in_specs=[smem] * 3 + [vmem] * 5,
        out_specs=(vmem, vmem),
        scratch_shapes=[
            pltpu.VMEM((2, side, side), jnp.float32),
            pltpu.VMEM((modes, side, 2 * side), jnp.float32),
            pltpu.VMEM((2, side, side + LANES), jnp.float32),
            pltpu.VMEM((side, side), jnp.float32),
        ],
        compiler_params=pltpu.CompilerParams(vmem_limit_bytes=32 * 2**20),
        cost_estimate=pl.CostEstimate(flops=flops, bytes_accessed=10 * 2**20, transcendentals=0),
    )(rows, cols, count, extended, probe, magnitudes, forward, inverse)


def return_rims(object_grad, margin):
    from_left = shifted(object_grad[:, :, -margin:], "col", 1)
    from_right = shifted(object_grad[:, :, :margin], "col", -1)
    middle = object_grad[:, :, margin:-margin] + jnp.concatenate([from_left, from_right], axis=2)
    from_above = shifted(middle[:, -margin:, :], "row", 1)
    from_below = shifted(middle[:, :margin, :], "row", -1)
    return middle[:, margin:-margin, :] + jnp.concatenate([from_above, from_below], axis=1)


def on_device(object_field, probe, pos_rows, pos_cols, counts, magnitudes):
    modes, side = probe.shape[1], probe.shape[2]
    margin = side // 2
    forward, inverse = dft_tables(side)
    errors = []
    for sweep in range(ITERS):
        for batch in range(BATCHES):
            extended = padded(object_field, (("row", 1), ("col", 2)), margin)
            object_grad, sums = batch_sums(
                extended, probe, pos_rows[0, 0, batch], pos_cols[0, 0, batch], counts[0, 0, batch : batch + 1],
                magnitudes[0, 0, batch], forward, inverse,
            )
            probe_peak = jnp.max(jnp.sum(probe * probe, axis=(0, 1))) + tiny_value
            total = lax.psum(sums, ("row", "col"))
            interior = return_rims(object_grad, margin)
            object_field = object_field + object_rate / probe_peak * interior
            tail = 2 * modes * side
            power_total = jnp.sum(total[tail])
            errors.append(jnp.sum(total[tail + 1]))
            summed = total[:tail].reshape(probe.shape)
            probe = probe + probe_rate * side * side / power_total * summed
    return (object_field, probe, jnp.stack(errors))


def solution(mesh):
    return jax.shard_map(
        on_device,
        mesh=mesh,
        in_specs=(
            P(None, "row", "col"),
            P(),
            P("row", "col", None, None),
            P("row", "col", None, None),
            P("row", "col", None),
            P("row", "col", None, None, None, None),
        ),
        out_specs=(P(None, "row", "col"), P(), P()),
        check_vma=False,
    )
```

```python
import functools
import math

import jax
import jax.numpy as jnp
import numpy as np
from jax import lax
from jax.experimental import pallas as pl
from jax.experimental.pallas import tpu as pltpu
from jax.sharding import PartitionSpec as P

BATCHES = 2
ITERS = 2


object_rate = 0.9
probe_rate = 0.5
floor_value = 0.5
tiny_value = 1e-06

CHUNK = 64
LANES = 128
SUBLANES = 8


def shifted(value, axis, steps):
    count = lax.axis_size(axis)
    leading, last = (max(0, -steps), min(count, count - steps))
    return lax.ppermute(value, axis, [(source, source + steps) for source in range(leading, last)])


def padded(array, sides, width):
    for axis, dim in sides:
        length = array.shape[dim]
        last = lax.slice_in_dim(array, length - width, length, axis=dim)
        leading = lax.slice_in_dim(array, 0, width, axis=dim)
        before = shifted(last, axis, 1)
        after = shifted(leading, axis, -1)
        array = jnp.concatenate([before, array, after], axis=dim)
    return array


def dft_tables(side):
    index = np.arange(side)
    angles = (index[:, None] * index[None, :] % side) * (2.0 * math.pi / side)
    cosine = np.cos(angles) / math.sqrt(side)
    sine = np.sin(angles) / math.sqrt(side)
    forward_left = np.block([[cosine, sine], [-sine, cosine]])
    inverse_left = np.block([[cosine, -sine], [sine, cosine]])
    return (jnp.asarray(forward_left, jnp.bfloat16), jnp.asarray(inverse_left, jnp.bfloat16))


def batch_kernel(
    rows_ref, cols_ref, count_ref, ext_ref, probe_ref, mag_ref, fwd_ref, inv_ref,
    grad_ref, sums_ref, win, far, term, square,
):
    modes, side = probe_ref.shape[1], probe_ref.shape[2]
    wide, tall = side + LANES, CHUNK + SUBLANES
    tail = 2 * modes * side

    grad_ref[...] = jnp.zeros_like(grad_ref)
    sums_ref[...] = jnp.zeros_like(sums_ref)

    def visit(slot, carry):
        row, col = rows_ref[slot], cols_ref[slot]
        first = pl.multiple_of(row // SUBLANES * SUBLANES, SUBLANES)
        down = row - first
        block = pl.multiple_of(col // LANES * LANES, LANES)
        offset = col - block

        for comp in range(2):
            for start in range(0, side, CHUNK):
                piece = ext_ref[comp, pl.ds(first + start, tall), pl.ds(block, wide)]
                piece = pltpu.roll(piece, lax.rem(wide - offset, wide), 1)[:, :side]
                piece = pltpu.roll(piece, lax.rem(tall - down, tall), 0)[:CHUNK]
                win[comp, start : start + CHUNK, :] = piece
                power = jnp.sum(piece * piece, axis=0, keepdims=True)
                sums_ref[tail : tail + 1, :] += power

        for mode in range(modes):
            p_re, p_im = probe_ref[0, mode], probe_ref[1, mode]
            w_re, w_im = win[0], win[1]
            wave = jnp.concatenate(
                [
                    (p_re * w_re - p_im * w_im).astype(jnp.bfloat16),
                    (p_re * w_im + p_im * w_re).astype(jnp.bfloat16),
                ],
                axis=0,
            )
            half = jnp.dot(fwd_ref[...], wave, preferred_element_type=jnp.float32).astype(jnp.bfloat16)
            half = jnp.concatenate([half[:side], half[side:]], axis=1)
            field = jnp.dot(half, inv_ref[...], preferred_element_type=jnp.float32)
            far[mode] = field
            norm = field[:, :side] * field[:, :side] + field[:, side:] * field[:, side:]
            if mode == 0:
                square[...] = norm
            else:
                square[...] += norm

        for start in range(0, side, CHUNK):
            span = slice(start, start + CHUNK)
            modulus = jnp.sqrt(square[span, :])
            amplitude = mag_ref[slot, span, :]
            miss = modulus - amplitude
            sums_ref[tail + 1 : tail + 2, :] += jnp.sum(miss * miss, axis=0, keepdims=True)
            square[span, :] = amplitude / jnp.maximum(modulus, floor_value) - 1.0

        for mode in range(modes):
            factor = square[...]
            fix = jnp.concatenate(
                [
                    (far[mode, :, :side] * factor).astype(jnp.bfloat16),
                    (far[mode, :, side:] * factor).astype(jnp.bfloat16),
                ],
                axis=0,
            )
            half = jnp.dot(inv_ref[...], fix, preferred_element_type=jnp.float32).astype(jnp.bfloat16)
            half = jnp.concatenate([half[:side], half[side:]], axis=1)
            wave = jnp.dot(half, fwd_ref[...], preferred_element_type=jnp.float32)
            u_re, u_im = wave[:, :side], wave[:, side:]
            p_re, p_im = probe_ref[0, mode], probe_ref[1, mode]
            w_re, w_im = win[0], win[1]
            t_re = p_re * u_re + p_im * u_im
            t_im = p_re * u_im - p_im * u_re
            if mode == 0:
                term[0, :, :side] = t_re
                term[1, :, :side] = t_im
            else:
                term[0, :, :side] += t_re
                term[1, :, :side] += t_im
            at_re, at_im = mode * side, (modes + mode) * side
            sums_ref[at_re : at_re + side, :] += w_re * u_re + w_im * u_im
            sums_ref[at_im : at_im + side, :] += w_re * u_im - w_im * u_re

        for comp in range(2):
            for start in range(0, side, CHUNK):
                piece = term[comp, start : start + CHUNK, :]
                piece = pltpu.roll(piece, offset, 1)
                piece = jnp.concatenate([piece, jnp.zeros((SUBLANES, wide), jnp.float32)], axis=0)
                piece = pltpu.roll(piece, down, 0)
                grad_ref[comp, pl.ds(first + start, tall), pl.ds(block, wide)] += piece
        return carry

    term[:, :, side:] = jnp.zeros((2, side, LANES), jnp.float32)
    lax.fori_loop(0, count_ref[0], visit, 0)


def batch_sums(extended, probe, rows, cols, count, magnitudes, forward, inverse):
    modes, side = probe.shape[1], probe.shape[2]
    vmem = pl.BlockSpec(memory_space=pltpu.VMEM)
    smem = pl.BlockSpec(memory_space=pltpu.SMEM)
    flops = 2 * magnitudes.shape[0] * modes * 4 * 2 * side * side * 4 * side
    return pl.pallas_call(
        batch_kernel,
        out_shape=(
            jax.ShapeDtypeStruct(extended.shape, jnp.float32),
            jax.ShapeDtypeStruct((2 * modes * side + 8, side), jnp.float32),
        ),
        in_specs=[smem] * 3 + [vmem] * 5,
        out_specs=(vmem, vmem),
        scratch_shapes=[
            pltpu.VMEM((2, side, side), jnp.float32),
            pltpu.VMEM((modes, side, 2 * side), jnp.float32),
            pltpu.VMEM((2, side, side + LANES), jnp.float32),
            pltpu.VMEM((side, side), jnp.float32),
        ],
        compiler_params=pltpu.CompilerParams(vmem_limit_bytes=32 * 2**20),
        cost_estimate=pl.CostEstimate(flops=flops, bytes_accessed=10 * 2**20, transcendentals=0),
    )(rows, cols, count, extended, probe, magnitudes, forward, inverse)


def return_rims(object_grad, margin):
    from_left = shifted(object_grad[:, :, -margin:], "col", 1)
    from_right = shifted(object_grad[:, :, :margin], "col", -1)
    middle = object_grad[:, :, margin:-margin] + jnp.concatenate([from_left, from_right], axis=2)
    from_above = shifted(middle[:, -margin:, :], "row", 1)
    from_below = shifted(middle[:, :margin, :], "row", -1)
    return middle[:, margin:-margin, :] + jnp.concatenate([from_above, from_below], axis=1)


def on_device(object_field, probe, pos_rows, pos_cols, counts, magnitudes):
    modes, side = probe.shape[1], probe.shape[2]
    margin = side // 2
    forward, inverse = dft_tables(side)
    errors = []
    for sweep in range(ITERS):
        for batch in range(BATCHES):
            extended = padded(object_field, (("row", 1), ("col", 2)), margin)
            object_grad, sums = batch_sums(
                extended, probe, pos_rows[0, 0, batch], pos_cols[0, 0, batch], counts[0, 0, batch : batch + 1],
                magnitudes[0, 0, batch], forward, inverse,
            )
            probe_peak = jnp.max(jnp.sum(probe * probe, axis=(0, 1))) + tiny_value
            tail = 2 * modes * side
            scalars = lax.psum(jnp.sum(sums[tail : tail + 2], axis=1), ("row", "col"))
            summed = lax.psum(sums[:tail].reshape(probe.shape), ("row", "col"))
            interior = return_rims(object_grad, margin)
            object_field = object_field + object_rate / probe_peak * interior
            power_total = scalars[0]
            errors.append(scalars[1])
            probe = probe + probe_rate * side * side / power_total * summed
    return (object_field, probe, jnp.stack(errors))


def solution(mesh):
    return jax.shard_map(
        on_device,
        mesh=mesh,
        in_specs=(
            P(None, "row", "col"),
            P(),
            P("row", "col", None, None),
            P("row", "col", None, None),
            P("row", "col", None),
            P("row", "col", None, None, None, None),
        ),
        out_specs=(P(None, "row", "col"), P(), P()),
        check_vma=False,
    )
```
